512 devices in a mesh: row: 32 (over x, y), col: 16 (over z, core).
Axes of the slice: x: 4, y: 8, z: 8, core: 2. Of those that a mesh axis runs over, the one named last changes fastest.
Arguments:
- inverse_block: float32 [16384, 16384], P('row', 'col'), may hold values from -6 to 6
- tile_list: int32 [32], replicated, may hold values from 0 to 63, as said below
- panels: bfloat16 [3, 16384, 512], P(None, 'row'), may hold values from -0.0625 to 0.0625
- links: bfloat16 [2, 512, 512], P(None, 'col'), may hold values from -0.25 to 0.25
- diag_inverse: float32 [3, 512, 512], P(None, None, 'col'), may hold values from -6 to 6
Outputs:
- panel_inverse: float32 [3, 16384, 512], P(None, 'row', 'col')
- cross_inverse: float32 [2, 512, 512], P(None, None, 'col')
- diag_block: float32 [3, 512, 512], P(None, None, 'col')
The draws below stay inside these ranges and needn't reach their ends.
Inputs may be any that keep to these rules, and one draw needn't show every extreme that they name: `tile_list`: 32 different tile numbers in ascending order; for each g from 0 to 16 - 1, the aligned group of tiles g * (64 // 16) to (g + 1) * (64 // 16) - 1 holds at least one of them.
All inputs are finite; a program needn't handle non-finite values.
Results may differ from the reference program's by a relative error of at most 0.0003.
Values may be sent and summed in bfloat16 or wider, within the bound.
A program may use at most 64 MiB of HBM per device.

```python
import jax
import jax.numpy as jnp
from jax import lax

ORDER = 16384
TILE = 256
W = 512
LIST = 32
SUPER = 3
N_COL = 16


def draw_tile_list(key, part):
    tile_count = ORDER // TILE
    group = tile_count // N_COL
    key_heat, key_noise, key_first, key_order = jax.random.split(jax.random.fold_in(key, 11), 4)
    heat = jax.random.randint(key_heat, (N_COL,), 0, 4)
    places = jnp.arange(tile_count, dtype=jnp.int32)
    owners = places // group
    noise = jax.random.randint(key_noise, (tile_count,), 0, 4)
    first = jax.random.randint(key_first, (N_COL,), 0, group)
    forced = places % group == first[owners]
    scores = jnp.where(forced, 1000, noise + 3 * heat[owners])
    order = jax.random.permutation(key_order, tile_count)
    totals = scores * tile_count + order
    chosen = lax.top_k(totals, LIST)[1]
    return jnp.sort(chosen).astype(jnp.int32)


def levels(stream_key, shape, pieces, smallest, largest):
    loudness, own = 1.0, jax.random.fold_in(stream_key, 6)
    for dim, blocks in pieces:
        heights = jnp.exp(jax.random.uniform(jax.random.fold_in(own, dim), (blocks,), jnp.float32, smallest / len(pieces), largest / len(pieces)))
        loudness = loudness * jnp.repeat(heights, shape[dim] // blocks).reshape([-1 if axis == dim else 1 for axis in range(len(shape))])
    return loudness


def gaussian(own_key, shape, spread, limit, cuts=(), kind=jnp.bfloat16):
    entries = jax.random.normal(own_key, shape, jnp.float32) * spread
    if len(cuts) > 0:
        entries = levels(own_key, shape, cuts, -0.22, 0.18) * entries
    return jnp.clip(entries, min=-limit, max=limit).astype(kind)


def setup_inputs(seed: int = 0) -> dict:
    seeds = jax.random.split(jax.random.key(seed), 6)
    inverse_block = gaussian(seeds[0], (ORDER, ORDER), 1.0, 6.0, ((0, 32), (1, 16)), jnp.float32)
    tile_list = draw_tile_list(jax.random.fold_in(seeds[5], 71), 0)
    panels = gaussian(seeds[2], (SUPER, ORDER, W), (LIST * TILE) ** -0.5, 0.0625, ((1, 32),))
    links = gaussian(seeds[3], (SUPER - 1, W, W), W ** -0.5, 0.25, ((1, 16),))
    diag_inverse = gaussian(seeds[4], (SUPER, W, W), 1.0, 6.0, ((2, 16),), jnp.float32)
    return {"inverse_block": inverse_block, "tile_list": tile_list, "panels": panels, "links": links, "diag_inverse": diag_inverse}


precise = lax.Precision.HIGHEST


def product(left, right):
    return jnp.dot(left, right, precision=precise, preferred_element_type=jnp.float32)


def reference(inverse_block, tile_list, panels, links, diag_inverse):
    offsets = jnp.arange(TILE, dtype=jnp.int32)
    row_index = (tile_list[:, None].astype(jnp.int32) * TILE + offsets[None, :]).reshape(-1).astype(jnp.int32)
    resident = jnp.take(jnp.take(inverse_block, row_index, axis=0), row_index, axis=1)
    panel_list = []
    cross_list = []
    diag_list = []
    previous = None
    diag_prev = None
    for supernode in range(SUPER):
        factor = jnp.take(panels[supernode], row_index, axis=0).astype(jnp.float32)
        inner_sum = product(resident, factor)
        if supernode > 0:
            link_block = links[supernode - 1].astype(jnp.float32)
            inner_sum = inner_sum + product(previous, link_block)
            cross_block = -(product(previous.T, factor) + product(diag_prev, link_block))
        current = -inner_sum
        diag_now = diag_inverse[supernode] - product(factor.T, current)
        if supernode > 0:
            diag_now = diag_now - product(link_block.T, cross_block)
            cross_list.append(cross_block)
        full_panel = jnp.zeros((ORDER, W), jnp.float32).at[row_index].set(current)
        panel_list.append(full_panel)
        diag_list.append(diag_now)
        previous = current
        diag_prev = diag_now
    return jnp.stack(panel_list), jnp.stack(cross_list), jnp.stack(diag_list)
```

```python
import functools

import jax
import jax.numpy as jnp
from jax import lax
from jax.experimental import pallas as pl
from jax.experimental.pallas import tpu as pltpu
from jax.sharding import PartitionSpec as P

NX = 4
NY = 8
TILE = 256
SUPER = 3
f32 = jnp.float32
bf16 = jnp.bfloat16


def halves(value):
    high = value.astype(bf16)
    low = (value - high.astype(f32)).astype(bf16)
    return high, low


def dot(left, right):
    return lax.dot_general(left, right, (((1,), (0,)), ((), ())), preferred_element_type=f32)


def dot_t(left, right):
    return lax.dot_general(left, right, (((1,), (1,)), ((), ())), preferred_element_type=f32)


def left_dot(left, right):
    high, low = halves(left)
    both = dot(jnp.concatenate([high, low], axis=0), right)
    return both[: left.shape[0]] + both[left.shape[0] :]


def kernel(
    nz, nc, tiles, s_ref, p_ref, l_ref, d_ref, x_out, y_out, g_out,
    sh, sl, pt, xp, xh, xl, xsib, xs, xr, cf, ct, ap, ar, ax, ay, bb, ex, tb, tt, gx, ga, yx, yf,
    psa_s, psc_s, psx_s, psa_r, psx_r, c_s, c_r, cd_s, cd_r, d2_s, d2_r, z_s, z_r,
    ar_s, ar_r, ay_s, ay_r, ex_s, ex_r, t_s, t_r, ga_s, ga_r, yx_s, yx_r,
):
    rows, depth = s_ref.shape
    wide = p_ref.shape[2]
    wc = wide // nc
    lanes = wide // NX
    cx = nc // NX
    kb = depth // 2
    r = lax.axis_index("row")
    c = lax.axis_index("col")
    x, y = lax.div(r, NY), lax.rem(r, NY)
    z, core = lax.div(c, 2), lax.rem(c, 2)
    other = 1 - core
    xt, slot = lax.div(c, cx), lax.rem(c, cx)
    my_lanes = pl.ds(pl.multiple_of(x * lanes, lanes), lanes)

    def ring(at, step, size):
        return lax.rem(at + step, size)

    pending = []

    def send(src, dst, ssem, rsem, row, col, cond=None):
        copy = pltpu.make_async_remote_copy(
            src_ref=src, dst_ref=dst, send_sem=ssem, recv_sem=rsem,
            device_id={"row": row, "col": col}, device_id_type=pl.DeviceIdType.MESH,
        )
        if cond is None:
            copy.start()
        else:
            pl.when(cond)(copy.start)
        pending.append((cond, copy))

    def arrived(dst, rsem, cond=None):
        copy = pltpu.make_async_remote_copy(
            src_ref=dst, dst_ref=dst, send_sem=rsem, recv_sem=rsem,
            device_id={"row": r, "col": c}, device_id_type=pl.DeviceIdType.MESH,
        )
        if cond is None:
            copy.wait_recv()
        else:
            pl.when(cond)(copy.wait_recv)

    def x_row(step):
        return ring(x, step, NX) * NY + y

    def y_row(step):
        return x * NY + ring(y, step, NY)

    barrier = pltpu.get_barrier_semaphore()

    def greet(row, col):
        pl.semaphore_signal(barrier, inc=1, device_id={"row": row, "col": col}, device_id_type=pl.DeviceIdType.MESH)

    for i in range(1, NX):
        greet(x_row(i), c)
    for i in range(1, NY):
        greet(y_row(i), c)
    for i in range(1, nc):
        greet(r, ring(c, i, nc))

    @pl.when(xt != x)
    def _():
        for i in range(cx):
            greet(xt * NY + y, x * cx + i)

    lane = lax.broadcasted_iota(jnp.int32, (1, rows), 1)
    mask = jnp.zeros((1, rows), f32)
    for j in range(rows // TILE):
        tile = r * (rows // TILE) + j
        hit = jnp.float32(0)
        for i in range(tiles.shape[0]):
            hit = hit + jnp.where(tiles[i] == tile, 1.0, 0.0)
        inside = jnp.where((lane >= j * TILE) & (lane < (j + 1) * TILE), 1.0, 0.0)
        mask = mask + inside * hit

    sources = [2 * c, 2 * c + 1]
    is_source = [r == src for src in sources]
    xq = [lax.div(src, NY) for src in sources]
    yq = [lax.rem(src, NY) for src in sources]
    dist = [lax.rem(y - yq[s] + NY, NY) for s in range(2)]

    for s in range(2):

        @pl.when(is_source[s])
        def _():
            for k in range(SUPER):
                turned = p_ref[k].T * mask.astype(bf16)
                pt[k, s] = turned.reshape(NX, lanes, kb)

    pl.semaphore_wait(barrier, NX - 1 + NY - 1 + nc - 1 + jnp.where(xt != x, cx, 0))

    for k in range(SUPER):
        for s in range(2):
            for i in range(1, NX):
                q = ring(x, i, NX)
                send(pt.at[k, s, q], pt.at[k, s, q], psc_s.at[k, s, i], psa_r.at[k, s], x_row(i), c, is_source[s])

    for i in range(1, nz):
        send(l_ref, cf.at[:, z, core], c_s.at[i], c_r.at[i], r, ring(z, i, nz) * 2 + core)
    cf[:, z, core] = l_ref[...]

    @pl.loop(0, rows // 128 if rows % 128 == 0 else 1)
    def _(j):
        size = 128 if rows % 128 == 0 else rows
        here = pl.ds(pl.multiple_of(j * size, size), size)
        for s in range(2):
            high, low = halves(s_ref[here, s * kb : (s + 1) * kb])
            sh[s, here] = high
            sl[s, here] = low

    def pass_on(k):
        for s in range(2):
            here = pt.at[k, s, x]
            arrived(here, psa_r.at[k, s], jnp.logical_not(is_source[s]))
            send(here, here, psa_s.at[k, s, 0], psa_r.at[k, s], y_row(1), c, dist[s] < NY // 2)
            down = (dist[s] == 0) | (dist[s] > NY // 2 + 1)
            send(here, here, psa_s.at[k, s, 1], psa_r.at[k, s], y_row(NY - 1), c, down)
            for i in range(1, NX):
                to_source = (dist[s] == 0) & (ring(x, i, NX) == xq[s])
                send(here, here, psx_s.at[k, s, i], psx_r.at[k, s, i], x_row(i), c, jnp.logical_not(to_source))

    def panel_here(k):
        for s in range(2):
            for i in range(1, NX):
                arrived(pt.at[k, s, ring(x, NX - i, NX)], psx_r.at[k, s, i], jnp.logical_not(is_source[s]))

    zx = nz // NX

    def partial(k):
        @pl.loop(0, NX)
        def _(q):
            acc = dot_t(pt[k, 0, q], sh[0]) + dot_t(pt[k, 0, q], sl[0])
            acc = acc + dot_t(pt[k, 1, q], sh[1]) + dot_t(pt[k, 1, q], sl[1])
            if k > 0:
                acc = acc + dot(ct[k - 1, q], xh[k - 1]) + dot(ct[k - 1, q], xl[k - 1])
            acc = -acc
            if k + 1 < SUPER:
                here = pl.ds(pl.multiple_of(q * lanes, lanes), lanes)
                high, low = halves(acc)
                xh[k, here] = high
                xl[k, here] = low
            xp[k, pl.ds(q * zx, zx)] = acc.reshape(zx, 2, wc, rows)

        send(xp.at[k, :, other], xsib.at[k], d2_s.at[k], d2_r.at[k], r, z * 2 + other)

    def along_z(k):
        arrived(xsib.at[k], d2_r.at[k])
        xs[k] = xp[k, :, core] + xsib[k]
        for i in range(1, nz):
            to = ring(z, i, nz)
            send(xs.at[k, to], xr.at[k, z], z_s.at[k, i], z_r.at[k, i], r, to * 2 + core)

    def summed(k):
        return wc if k + 1 == SUPER else 2 * wc

    def inverse_panel(k):
        total = xs[k, z]
        for i in range(1, nz):
            src = ring(z, nz - i, nz)
            arrived(xr.at[k, src], z_r.at[k, i])
            total = total + xr[k, src]
        total = total * mask
        x_out[k] = total
        high, low = halves(total)
        both = jnp.concatenate([high, low], axis=0)
        for j in range(k, min(k + 2, SUPER)):
            terms = dot(both, p_ref[j])
            at = (j - k) * wc
            ap[k, at : at + wc] = terms[:wc] + terms[wc:]
        n = summed(k)
        for i in range(1, NX):
            to = ring(x, i, NX)
            cut = pl.ds(pl.multiple_of(to * lanes, lanes), lanes)
            send(ap.at[k, :n, cut], ar.at[k, x, :n], ar_s.at[k, i], ar_r.at[k, i], x_row(i), c)

    def along_y(k):
        n = summed(k)
        total = ap[k, :n, my_lanes]
        for i in range(1, NX):
            src = ring(x, NX - i, NX)
            arrived(ar.at[k, src, :n], ar_r.at[k, i])
            total = total + ar[k, src, :n]
        ax[k, :n] = total
        for i in range(1, NY):
            send(ax.at[k, :n], ay.at[k, y, :n], ay_s.at[k, i], ay_r.at[k, i], y_row(i), c)

    def products(k):
        n = summed(k)
        total = ax[k, :n]
        for i in range(1, NY):
            src = ring(y, NY - i, NY)
            arrived(ay.at[k, src, :n], ay_r.at[k, i])
            total = total + ay[k, src, :n]
        bb[k, :n] = total
        ex[k, :, my_lanes] = total[:wc]
        for i in range(1, NX):
            send(bb.at[k, :wc], ex.at[k, :, my_lanes], ex_s.at[k, i], ex_r.at[k, i], x_row(i), c)
        if k + 1 < SUPER:
            for i in range(cx):
                away = (xt != x) | (slot != i)
                send(bb.at[k, wc:], tb.at[k, slot], t_s.at[k, i], t_r.at[k, slot], xt * NY + y, x * cx + i, away)

                @pl.when(jnp.logical_not(away))
                def _():
                    tb[k, i] = bb[k, wc:]

    def everyone(k):
        ga[k, c] = gx[k]
        for i in range(1, nc):
            send(gx.at[k], ga.at[k, c], ga_s.at[k, i], ga_r.at[k, i], r, ring(c, i, nc))

    def cross(k):
        for i in range(cx):
            arrived(tb.at[k, i], t_r.at[k, i], (xt != x) | (slot != i))
        tt[...] = tb[k].reshape(cx * wc, lanes).T.reshape(cx, wc, lanes)
        for i in range(1, nc):
            arrived(ga.at[k, ring(c, nc - i, nc)], ga_r.at[k, i])
        high, low = halves(ga[k].reshape(nc * wc, lanes))
        factor = ct[k, xt, pl.ds(pl.multiple_of(slot * wc, wc), wc)]
        block = -(tt[slot] + dot(factor, high) + dot(factor, low))
        yx[k] = block
        yf[k, :, my_lanes] = block
        for i in range(1, NX):
            send(yx.at[k], yf.at[k, :, my_lanes], yx_s.at[k, i], yx_r.at[k, i], x_row(i), c)

    def lanes_of(step):
        return pl.ds(pl.multiple_of(ring(x, step, NX) * lanes, lanes), lanes)

    def gathered(ref, sems, k):
        for i in range(1, NX):
            arrived(ref.at[k, :, lanes_of(NX - i)], sems.at[k, i])
        return ref[k]

    pass_on(0)
    pass_on(1)
    panel_here(0)
    partial(0)
    pass_on(2)
    along_z(0)

    for i in range(1, nz):
        arrived(cf.at[:, ring(z, nz - i, nz), core], c_r.at[i])
    send(cf.at[:, :, core], cf.at[:, :, core], cd_s.at[0], cd_r.at[0], r, z * 2 + other)
    arrived(cf.at[:, :, other], cd_r.at[0])
    for k in range(SUPER - 1):
        ct[k] = cf[k].reshape(wide, wide).T.reshape(NX, lanes, wide)

    panel_here(1)
    partial(1)
    inverse_panel(0)
    along_z(1)
    along_y(0)
    panel_here(2)
    partial(2)
    products(0)
    along_z(2)
    gx[0] = d_ref[0, :, my_lanes] - bb[0, :wc]
    everyone(0)
    inverse_panel(1)
    along_y(1)
    cross(0)
    inverse_panel(2)
    g_out[0] = d_ref[0] - gathered(ex, ex_r, 0)
    products(1)
    y_out[0] = gathered(yf, yx_r, 0)
    along_y(2)
    g_out[1] = d_ref[1] - gathered(ex, ex_r, 1) - left_dot(y_out[0], cf[0].reshape(wide, wide))
    gx[1] = g_out[1, :, my_lanes]
    everyone(1)
    products(2)
    cross(1)
    y_out[1] = gathered(yf, yx_r, 1)
    g_out[2] = d_ref[2] - gathered(ex, ex_r, 2) - left_dot(y_out[1], cf[1].reshape(wide, wide))

    for cond, copy in pending:
        if cond is None:
            copy.wait_send()
        else:
            pl.when(cond)(copy.wait_send)


def local(nz, nc, inverse_block, tile_list, panels, links, diag_inverse):
    rows, depth = inverse_block.shape
    wide = panels.shape[2]
    wc = wide // nc
    lanes = wide // NX
    cx = nc // NX
    pair = SUPER - 1
    vmem = pl.BlockSpec(memory_space=pltpu.VMEM)
    dma = pltpu.SemaphoreType.DMA
    x, y, g = pl.pallas_call(
        functools.partial(kernel, nz, nc),
        out_shape=(
            jax.ShapeDtypeStruct((SUPER, wc, rows), f32),
            jax.ShapeDtypeStruct((pair, wc, wide), f32),
            jax.ShapeDtypeStruct((SUPER, wc, wide), f32),
        ),
        in_specs=[pl.BlockSpec(memory_space=pltpu.SMEM), vmem, vmem, vmem, vmem],
        out_specs=(vmem, vmem, vmem),
        scratch_shapes=[
            pltpu.VMEM((2, rows, depth // 2), bf16),
            pltpu.VMEM((2, rows, depth // 2), bf16),
            pltpu.VMEM((SUPER, 2, NX, lanes, depth // 2), bf16),
            pltpu.VMEM((SUPER, nz, 2, wc, rows), f32),
            pltpu.VMEM((pair, wide, rows), bf16),
            pltpu.VMEM((pair, wide, rows), bf16),
            pltpu.VMEM((SUPER, nz, wc, rows), f32),
            pltpu.VMEM((SUPER, nz, wc, rows), f32),
            pltpu.VMEM((SUPER, nz, wc, rows), f32),
            pltpu.VMEM((pair, nz, 2, wc, wide), bf16),
            pltpu.VMEM((pair, NX, lanes, wide), bf16),
            pltpu.VMEM((SUPER, 2 * wc, wide), f32),
            pltpu.VMEM((SUPER, NX, 2 * wc, lanes), f32),
            pltpu.VMEM((SUPER, 2 * wc, lanes), f32),
            pltpu.VMEM((SUPER, NY, 2 * wc, lanes), f32),
            pltpu.VMEM((SUPER, 2 * wc, lanes), f32),
            pltpu.VMEM((SUPER, wc, wide), f32),
            pltpu.VMEM((pair, cx, wc, lanes), f32),
            pltpu.VMEM((cx, wc, lanes), f32),
            pltpu.VMEM((pair, wc, lanes), f32),
            pltpu.VMEM((pair, nc, wc, lanes), f32),
            pltpu.VMEM((pair, wc, lanes), f32),
            pltpu.VMEM((pair, wc, wide), f32),
            dma((SUPER, 2, 2)),
            dma((SUPER, 2, NX)),
            dma((SUPER, 2, NX)),
            dma((SUPER, 2)),
            dma((SUPER, 2, NX)),
            dma((nz,)), dma((nz,)),
            dma((1,)), dma((1,)),
            dma((SUPER,)), dma((SUPER,)),
            dma((SUPER, nz)), dma((SUPER, nz)),
            dma((SUPER, NX)), dma((SUPER, NX)),
            dma((SUPER, NY)), dma((SUPER, NY)),
            dma((SUPER, NX)), dma((SUPER, NX)),
            dma((pair, cx)), dma((pair, cx)),
            dma((pair, nc)), dma((pair, nc)),
            dma((pair, NX)), dma((pair, NX)),
        ],
        compiler_params=pltpu.CompilerParams(
            collective_id=0, has_side_effects=True, vmem_limit_bytes=60 * 1024 * 1024
        ),
    )(tile_list, inverse_block, panels, links, jnp.swapaxes(diag_inverse, 1, 2))
    return tuple(jnp.swapaxes(value, 1, 2) for value in (x, y, g))


def solution(mesh):
    nc = mesh.shape["col"]
    return jax.shard_map(
        functools.partial(local, nc // 2, nc),
        mesh=mesh,
        in_specs=(
            P("row", "col"),
            P(),
            P(None, "row", None),
            P(None, "col", None),
            P(None, None, "col"),
        ),
        out_specs=(P(None, "row", "col"), P(None, None, "col"), P(None, None, "col")),
        check_vma=False,
    )
```

```python
import functools

import jax
import jax.numpy as jnp
from jax import lax
from jax.experimental import pallas as pl
from jax.experimental.pallas import tpu as pltpu
from jax.sharding import PartitionSpec as P

NX = 4
NY = 8
TILE = 256
SUPER = 3
f32 = jnp.float32
bf16 = jnp.bfloat16


def halves(value):
    high = value.astype(bf16)
    low = (value - high.astype(f32)).astype(bf16)
    return high, low


def dot(left, right):
    return lax.dot_general(left, right, (((1,), (0,)), ((), ())), preferred_element_type=f32)


def dot_t(left, right):
    return lax.dot_general(left, right, (((1,), (1,)), ((), ())), preferred_element_type=f32)


def left_dot(left, right):
    high, low = halves(left)
    both = dot(jnp.concatenate([high, low], axis=0), right)
    return both[: left.shape[0]] + both[left.shape[0] :]


def along(size):
    if size == 8:
        return (((0,), 3), ((0, 1, 3), 1), ((0,), 6), ((0, 6), 7))
    return (((0, 1), 1), ((0,), 3))


def any_of(value, choices):
    hit = value == choices[0]
    for choice in choices[1:]:
        hit = hit | (value == choice)
    return hit


def kernel(
    nz, nc, tiles, s_hbm, p_hbm, l_hbm, d_hbm, x_out, y_out, g_out,
    s_ref, p_ref, l_ref, d_ref, in_s,
    sh, sl, pt, xp, xh, xl, xsib, xs, xr, own, sc, sr, cf, ct, ap, ar, ax, ay, bb, ex, tb, tt, gx, ga, yx, yf,
    psa_s, psc_s, psx_s, psa_r, psx_r, c_s, c_r, cd_s, cd_r, d2_s, d2_r, z_s, z_r, s_s, s_r,
    ar_s, ar_r, ay_s, ay_r, ex_s, ex_r, t_s, t_r, ga_s, ga_r, gd_s, gd_r, yx_s, yx_r,
):
    rows, depth = s_ref.shape
    wide = p_ref.shape[2]
    wc = wide // nc
    lanes = wide // NX
    cx = nc // NX
    kb = depth // 2
    r = lax.axis_index("row")
    c = lax.axis_index("col")
    x, y = lax.div(r, NY), lax.rem(r, NY)
    z, core = lax.div(c, 2), lax.rem(c, 2)
    other = 1 - core
    xt, slot = lax.div(c, cx), lax.rem(c, cx)
    my_lanes = pl.ds(pl.multiple_of(x * lanes, lanes), lanes)

    def ring(at, step, size):
        return lax.rem(at + step, size)

    pending = []

    def send(src, dst, ssem, rsem, row, col, cond=None):
        copy = pltpu.make_async_remote_copy(
            src_ref=src, dst_ref=dst, send_sem=ssem, recv_sem=rsem,
            device_id={"row": row, "col": col}, device_id_type=pl.DeviceIdType.MESH,
        )
        if cond is None:
            copy.start()
        else:
            pl.when(cond)(copy.start)
        pending.append((cond, copy))

    def arrived(dst, rsem, cond=None):
        copy = pltpu.make_async_remote_copy(
            src_ref=dst, dst_ref=dst, send_sem=rsem, recv_sem=rsem,
            device_id={"row": r, "col": c}, device_id_type=pl.DeviceIdType.MESH,
        )
        if cond is None:
            copy.wait_recv()
        else:
            pl.when(cond)(copy.wait_recv)

    def x_row(step):
        return ring(x, step, NX) * NY + y

    def y_row(step):
        return x * NY + ring(y, step, NY)

    loads = [
        pltpu.make_async_copy(src, dst, in_s.at[i])
        for i, (src, dst) in enumerate(((p_hbm, p_ref), (l_hbm, l_ref), (s_hbm, s_ref), (d_hbm, d_ref)))
    ]
    for load in loads:
        load.start()

    barrier = pltpu.get_barrier_semaphore()

    def greet(row, col):
        pl.semaphore_signal(barrier, inc=1, device_id={"row": row, "col": col}, device_id_type=pl.DeviceIdType.MESH)

    for i in range(1, NX):
        greet(x_row(i), c)
    for i in range(1, NY):
        greet(y_row(i), c)
    for i in range(1, nc):
        greet(r, ring(c, i, nc))

    @pl.when(xt != x)
    def _():
        for i in range(cx):
            greet(xt * NY + y, x * cx + i)

    lane = lax.broadcasted_iota(jnp.int32, (1, rows), 1)
    mask = jnp.zeros((1, rows), f32)
    for j in range(rows // TILE):
        tile = r * (rows // TILE) + j
        hit = jnp.float32(0)
        for i in range(tiles.shape[0]):
            hit = hit + jnp.where(tiles[i] == tile, 1.0, 0.0)
        inside = jnp.where((lane >= j * TILE) & (lane < (j + 1) * TILE), 1.0, 0.0)
        mask = mask + inside * hit

    sources = [2 * c, 2 * c + 1]
    dist = [lax.rem(y - lax.rem(src, NY) + NY, NY) for src in sources]
    near = jnp.where(dist[1] < dist[0], 1, 0)
    order = []
    for src in (near, 1 - near):
        at = 2 * c + src
        xs_at = lax.div(at, NY)
        order.append((src, r == at, lax.rem(y - lax.rem(at, NY) + NY, NY), xs_at))

    loads[0].wait()
    for s in range(2):

        @pl.when(r == sources[s])
        def _():
            for k in range(SUPER):
                turned = p_ref[k].T * mask.astype(bf16)
                pt[k, s] = turned.reshape(NX, 2, lanes // 2, kb)

    pl.semaphore_wait(barrier, NX - 1 + NY - 1 + nc - 1 + jnp.where(xt != x, cx, 0))

    def inject(k):
        for s, is_source, _, _ in order[:1]:
            for h in range(2):
                for i in (2, 1, 3) if NX == 4 else range(1, NX):
                    q = ring(x, i, NX)
                    here = pt.at[k, s, q, h]
                    send(here, here, psc_s.at[k, h, i], psa_r.at[k, s, h], x_row(i), c, is_source)

    def pass_on(k):
        for j, (s, is_source, away, xq) in enumerate(order):
            for h in range(2):
                here = pt.at[k, s, x, h]
                arrived(here, psa_r.at[k, s, h], jnp.logical_not(is_source))
                for n, (senders, step) in enumerate(along(NY)):
                    send(here, here, psa_s.at[k, j, h, n], psa_r.at[k, s, h], y_row(step), c, any_of(away, senders))
                for i in (1, NX - 1) if NX > 2 else (1,):
                    to_source = (away == 0) & (ring(x, i, NX) == xq)
                    send(
                        here, here, psx_s.at[k, j, h, i], psx_r.at[k, s, h, i], x_row(i), c, jnp.logical_not(to_source)
                    )

    def forward(k):
        for j, (s, is_source, away, xq) in enumerate(order):
            needed = jnp.logical_not(is_source)
            for h in range(2):
                for i in (1, NX - 1) if NX > 2 else (1,):
                    there = pt.at[k, s, ring(x, NX - i, NX), h]
                    arrived(there, psx_r.at[k, s, h, i], needed)
                    if NX == 4 and i == (1 if h == 0 else 3):
                        to_source = (away == 0) & (ring(x, i, NX) == xq)
                        send(
                            there, there, psx_s.at[k, j, h, 2], psx_r.at[k, s, h, 2], x_row(i), c,
                            jnp.logical_not(to_source),
                        )

    def panel_here(k):
        if NX == 4:
            for s, is_source, _, _ in order:
                for h in range(2):
                    arrived(pt.at[k, s, ring(x, 2, NX), h], psx_r.at[k, s, h, 2], jnp.logical_not(is_source))

    def two_terms():
        loads[2].wait()
        size = min(rows, 128)

        @pl.loop(0, rows // size)
        def _(j):
            here = pl.ds(pl.multiple_of(j * size, size), size)
            for s in range(2):
                high, low = halves(s_ref[here, s * kb : (s + 1) * kb])
                sh[s, here] = high
                sl[s, here] = low

    def share_links():
        loads[1].wait()
        for i in range(1, nz):
            send(l_ref, cf.at[:, z, core], c_s.at[i], c_r.at[i], r, ring(z, i, nz) * 2 + core)
        cf[:, z, core] = l_ref[...]

    zx = nz // NX

    def partial(k):
        two = 2 * lanes

        @pl.loop(0, NX // 2)
        def _(q):
            first = pt[k, 0, pl.ds(2 * q, 2)].reshape(two, kb)
            second = pt[k, 1, pl.ds(2 * q, 2)].reshape(two, kb)
            acc = dot_t(first, sh[0]) + dot_t(first, sl[0])
            acc = acc + dot_t(second, sh[1]) + dot_t(second, sl[1])
            if k > 0:
                factor = ct[k - 1, pl.ds(2 * q, 2)].reshape(two, wide)
                acc = acc + dot(factor, xh[k - 1]) + dot(factor, xl[k - 1])
            acc = -acc
            if k + 1 < SUPER:
                here = pl.ds(pl.multiple_of(q * two, two), two)
                high, low = halves(acc)
                xh[k, here] = high
                xl[k, here] = low
            xp[k, pl.ds(q * 2 * zx, 2 * zx)] = acc.reshape(2 * zx, 2, wc, rows)

        send(xp.at[k, :, other], xsib.at[k], d2_s.at[k], d2_r.at[k], r, z * 2 + other)

    def along_z(k):
        arrived(xsib.at[k], d2_r.at[k])
        mine = xp[k, :, core] + xsib[k]
        own[k] = xp[k, z, core] + xsib[k, z]
        top = jnp.max(jnp.abs(mine), axis=1, keepdims=True)
        sc[k] = top * (1 / 32767)
        steps = jnp.where(top > 0, 32767 / jnp.where(top > 0, top, 1.0), 0.0)
        xs[k] = jnp.round(mine * steps).astype(jnp.int32).astype(jnp.int16)
        for i in range(1, nz):
            to = ring(z, i, nz)
            send(sc.at[k, to], sr.at[k, z], s_s.at[k, i], s_r.at[k, i], r, to * 2 + core)
            send(xs.at[k, to], xr.at[k, z], z_s.at[k, i], z_r.at[k, i], r, to * 2 + core)

    def summed(k):
        return wc if k + 1 == SUPER else 2 * wc

    def inverse_panel(k):
        total = own[k]
        for i in range(1, nz):
            src = ring(z, nz - i, nz)
            arrived(sr.at[k, src], s_r.at[k, i])
            arrived(xr.at[k, src], z_r.at[k, i])
            total = total + xr[k, src].astype(jnp.int32).astype(f32) * sr[k, src]
        total = total * mask
        x_out[k] = total
        high, low = halves(total)
        both = jnp.concatenate([high, low], axis=0)
        for j in range(k, min(k + 2, SUPER)):
            terms = dot(both, p_ref[j])
            at = (j - k) * wc
            ap[k, at : at + wc] = terms[:wc] + terms[wc:]
        n = summed(k)
        for i in range(1, NX):
            to = ring(x, i, NX)
            cut = pl.ds(pl.multiple_of(to * lanes, lanes), lanes)
            send(ap.at[k, :n, cut], ar.at[k, x, :n], ar_s.at[k, i], ar_r.at[k, i], x_row(i), c)

    def along_y(k):
        n = summed(k)
        total = ap[k, :n, my_lanes]
        for i in range(1, NX):
            src = ring(x, NX - i, NX)
            arrived(ar.at[k, src, :n], ar_r.at[k, i])
            total = total + ar[k, src, :n]
        ax[k, :n] = total
        for i in range(1, NY):
            send(ax.at[k, :n], ay.at[k, y, :n], ay_s.at[k, i], ay_r.at[k, i], y_row(i), c)

    def products(k):
        n = summed(k)
        total = ax[k, :n]
        for i in range(1, NY):
            src = ring(y, NY - i, NY)
            arrived(ay.at[k, src, :n], ay_r.at[k, i])
            total = total + ay[k, src, :n]
        bb[k, :n] = total
        ex[k, :, my_lanes] = total[:wc]
        for i in range(1, NX):
            send(bb.at[k, :wc], ex.at[k, :, my_lanes], ex_s.at[k, i], ex_r.at[k, i], x_row(i), c)
        if k + 1 < SUPER:
            for i in range(cx):
                away = (xt != x) | (slot != i)
                send(bb.at[k, wc:], tb.at[k, slot], t_s.at[k, i], t_r.at[k, slot], xt * NY + y, x * cx + i, away)

                @pl.when(jnp.logical_not(away))
                def _():
                    tb[k, i] = bb[k, wc:]

    def everyone(k):
        for i in range(1, nz):
            send(gx.at[k], ga.at[k, z, core], ga_s.at[k, i], ga_r.at[k, i], r, ring(z, i, nz) * 2 + core)
        ga[k, z, core] = gx[k]

    def cross(k):
        for i in range(1, nz):
            arrived(ga.at[k, ring(z, nz - i, nz), core], ga_r.at[k, i])
        send(ga.at[k, :, core], ga.at[k, :, core], gd_s.at[k], gd_r.at[k], r, z * 2 + other)
        for i in range(cx):
            arrived(tb.at[k, i], t_r.at[k, i], (xt != x) | (slot != i))
        tt[...] = tb[k].reshape(cx * wc, lanes).T.reshape(cx, wc, lanes)
        arrived(ga.at[k, :, other], gd_r.at[k])
        high, low = halves(ga[k].reshape(nc * wc, lanes))
        factor = ct[k, xt, pl.ds(pl.multiple_of(slot * wc, wc), wc)]
        block = -(tt[slot] + dot(factor, high) + dot(factor, low))
        yx[k] = block
        yf[k, :, my_lanes] = block
        for i in range(1, NX):
            send(yx.at[k], yf.at[k, :, my_lanes], yx_s.at[k, i], yx_r.at[k, i], x_row(i), c)

    def lanes_of(step):
        return pl.ds(pl.multiple_of(ring(x, step, NX) * lanes, lanes), lanes)

    def gathered(ref, sems, k):
        for i in range(1, NX):
            arrived(ref.at[k, :, lanes_of(NX - i)], sems.at[k, i])
        return ref[k]

    inject(0)
    share_links()
    pass_on(0)
    inject(1)
    two_terms()
    forward(0)
    pass_on(1)
    inject(2)
    panel_here(0)
    partial(0)
    forward(1)
    pass_on(2)
    along_z(0)

    for i in range(1, nz):
        arrived(cf.at[:, ring(z, nz - i, nz), core], c_r.at[i])
    send(cf.at[:, :, core], cf.at[:, :, core], cd_s.at[0], cd_r.at[0], r, z * 2 + other)
    arrived(cf.at[:, :, other], cd_r.at[0])
    for k in range(SUPER - 1):
        ct[k] = cf[k].reshape(wide, wide).T.reshape(NX, lanes, wide)

    panel_here(1)
    partial(1)
    forward(2)
    along_z(1)
    inverse_panel(0)
    panel_here(2)
    partial(2)
    along_y(0)
    along_z(2)
    loads[3].wait()
    inverse_panel(1)
    products(0)
    gx[0] = d_ref[0, :, my_lanes] - bb[0, :wc]
    everyone(0)
    along_y(1)
    inverse_panel(2)
    cross(0)
    g_out[0] = d_ref[0] - gathered(ex, ex_r, 0)
    products(1)
    along_y(2)
    y_out[0] = gathered(yf, yx_r, 0)
    g_out[1] = d_ref[1] - gathered(ex, ex_r, 1) - left_dot(y_out[0], cf[0].reshape(wide, wide))
    gx[1] = g_out[1, :, my_lanes]
    everyone(1)
    products(2)
    cross(1)
    y_out[1] = gathered(yf, yx_r, 1)
    g_out[2] = d_ref[2] - gathered(ex, ex_r, 2) - left_dot(y_out[1], cf[1].reshape(wide, wide))

    for cond, copy in pending:
        if cond is None:
            copy.wait_send()
        else:
            pl.when(cond)(copy.wait_send)


def finish(x_ref, y_ref, g_ref, x_out, y_out, g_out):
    x_out[...] = x_ref[...]
    y_out[...] = y_ref[...]
    g_out[...] = g_ref[...]


def local(nz, nc, inverse_block, tile_list, panels, links, diag_inverse):
    rows, depth = inverse_block.shape
    wide = panels.shape[2]
    wc = wide // nc
    lanes = wide // NX
    cx = nc // NX
    pair = SUPER - 1
    vmem = pl.BlockSpec(memory_space=pltpu.VMEM)
    dma = pltpu.SemaphoreType.DMA
    x, y, g = pl.pallas_call(
        functools.partial(kernel, nz, nc),
        out_shape=(
            jax.ShapeDtypeStruct((SUPER, wc, rows), f32),
            jax.ShapeDtypeStruct((pair, wc, wide), f32),
            jax.ShapeDtypeStruct((SUPER, wc, wide), f32),
        ),
        in_specs=[pl.BlockSpec(memory_space=pltpu.SMEM)] + [pl.BlockSpec(memory_space=pl.ANY)] * 4,
        out_specs=(vmem, vmem, vmem),
        scratch_shapes=[
            pltpu.VMEM((rows, depth), f32),
            pltpu.VMEM(panels.shape, bf16),
            pltpu.VMEM(links.shape, bf16),
            pltpu.VMEM((SUPER, wc, wide), f32),
            dma((4,)),
            pltpu.VMEM((2, rows, depth // 2), bf16),
            pltpu.VMEM((2, rows, depth // 2), bf16),
            pltpu.VMEM((SUPER, 2, NX, 2, lanes // 2, depth // 2), bf16),
            pltpu.VMEM((SUPER, nz, 2, wc, rows), f32),
            pltpu.VMEM((pair, wide, rows), bf16),
            pltpu.VMEM((pair, wide, rows), bf16),
            pltpu.VMEM((SUPER, nz, wc, rows), f32),
            pltpu.VMEM((SUPER, nz, wc, rows), jnp.int16),
            pltpu.VMEM((SUPER, nz, wc, rows), jnp.int16),
            pltpu.VMEM((SUPER, wc, rows), f32),
            pltpu.VMEM((SUPER, nz, 1, rows), f32),
            pltpu.VMEM((SUPER, nz, 1, rows), f32),
            pltpu.VMEM((pair, nz, 2, wc, wide), bf16),
            pltpu.VMEM((pair, NX, lanes, wide), bf16),
            pltpu.VMEM((SUPER, 2 * wc, wide), f32),
            pltpu.VMEM((SUPER, NX, 2 * wc, lanes), f32),
            pltpu.VMEM((SUPER, 2 * wc, lanes), f32),
            pltpu.VMEM((SUPER, NY, 2 * wc, lanes), f32),
            pltpu.VMEM((SUPER, 2 * wc, lanes), f32),
            pltpu.VMEM((SUPER, wc, wide), f32),
            pltpu.VMEM((pair, cx, wc, lanes), f32),
            pltpu.VMEM((cx, wc, lanes), f32),
            pltpu.VMEM((pair, wc, lanes), f32),
            pltpu.VMEM((pair, nz, 2, wc, lanes), f32),
            pltpu.VMEM((pair, wc, lanes), f32),
            pltpu.VMEM((pair, wc, wide), f32),
            dma((SUPER, 2, 2, len(along(NY)))),
            dma((SUPER, 2, NX)),
            dma((SUPER, 2, 2, NX)),
            dma((SUPER, 2, 2)),
            dma((SUPER, 2, 2, NX)),
            dma((nz,)), dma((nz,)),
            dma((1,)), dma((1,)),
            dma((SUPER,)), dma((SUPER,)),
            dma((SUPER, nz)), dma((SUPER, nz)),
            dma((SUPER, nz)), dma((SUPER, nz)),
            dma((SUPER, NX)), dma((SUPER, NX)),
            dma((SUPER, NY)), dma((SUPER, NY)),
            dma((SUPER, NX)), dma((SUPER, NX)),
            dma((pair, cx)), dma((pair, cx)),
            dma((pair, nz)), dma((pair, nz)),
            dma((pair,)), dma((pair,)),
            dma((pair, NX)), dma((pair, NX)),
        ],
        compiler_params=pltpu.CompilerParams(
            collective_id=0, has_side_effects=True, vmem_limit_bytes=60 * 1024 * 1024
        ),
    )(tile_list, inverse_block, panels, links, jnp.swapaxes(diag_inverse, 1, 2))
    x, y, g = pl.pallas_call(
        finish,
        out_shape=tuple(jax.ShapeDtypeStruct(value.shape, f32) for value in (x, y, g)),
        in_specs=[vmem] * 3,
        out_specs=(vmem,) * 3,
    )(x, y, g)
    return tuple(jnp.swapaxes(value, 1, 2) for value in (x, y, g))


def solution(mesh):
    nc = mesh.shape["col"]
    return jax.shard_map(
        functools.partial(local, nc // 2, nc),
        mesh=mesh,
        in_specs=(
            P("row", "col"),
            P(),
            P(None, "row", None),
            P(None, "col", None),
            P(None, None, "col"),
        ),
        out_specs=(P(None, "row", "col"), P(None, None, "col"), P(None, None, "col")),
        check_vma=False,
    )
```

```python
import functools

import jax
import jax.numpy as jnp
from jax import lax
from jax.experimental import pallas as pl
from jax.experimental.pallas import tpu as pltpu
from jax.sharding import PartitionSpec as P

NX = 4
NY = 8
TILE = 256
SUPER = 3
f32 = jnp.float32
bf16 = jnp.bfloat16


def halves(value):
    high = value.astype(bf16)
    low = (value - high.astype(f32)).astype(bf16)
    return high, low


def dot(left, right):
    return lax.dot_general(left, right, (((1,), (0,)), ((), ())), preferred_element_type=f32)


def dot_t(left, right):
    return lax.dot_general(left, right, (((1,), (1,)), ((), ())), preferred_element_type=f32)


def left_dot(left, right):
    high, low = halves(left)
    both = dot(jnp.concatenate([high, low], axis=0), right)
    return both[: left.shape[0]] + both[left.shape[0] :]


def along(size):
    if size == 8:
        return (((0,), 0, 0, 2), ((0,), 0, 0, 6), ((0, 2), 0, 3, 1), ((0, 6), 5, 0, 7))
    return (((0, 1), 0, 0, 1), ((0,), 0, 0, 3))


def any_of(value, choices):
    hit = value == choices[0]
    for choice in choices[1:]:
        hit = hit | (value == choice)
    return hit


def kernel(
    nz, nc, tiles, s_hbm, p_hbm, l_hbm, d_hbm, x_hbm, y_hbm, g_hbm,
    s_ref, p_ref, l_ref, d_ref, x_out, y_out, g_out, in_s, out_s,
    sh, sl, pt, xp, xh, xl, xsib, xs, xr, own, sc, sr, cf, ct, ap, ar, ax, ay, bb, ex, tb, tf, tt, gx, ga, ya, yx, yf, vc,
    psa_s, psc_s, psx_s, psa_r, psx_r, psf_r, c_s, c_r, cd_s, cd_r, d2_s, d2_r, z_s, z_r, s_s, s_r,
    ar_s, ar_r, ay_s, ay_r, ex_s, ex_r, t_s, t_r, tf_s, tf_r, td_s, td_r, ga_s, ga_r, gd_s, gd_r, yx_s, yx_r,
):
    rows, depth = s_ref.shape
    wide = p_ref.shape[2]
    wc = wide // nc
    lanes = wide // NX
    cx = nc // NX
    kb = depth // 2
    r = lax.axis_index("row")
    c = lax.axis_index("col")
    x, y = lax.div(r, NY), lax.rem(r, NY)
    z, core = lax.div(c, 2), lax.rem(c, 2)
    other = 1 - core
    xt, slot = lax.div(c, cx), lax.rem(c, cx)
    my_lanes = pl.ds(pl.multiple_of(x * lanes, lanes), lanes)

    def ring(at, step, size):
        return lax.rem(at + step, size)

    pending = []

    def send(src, dst, ssem, rsem, row, col, cond=None):
        copy = pltpu.make_async_remote_copy(
            src_ref=src, dst_ref=dst, send_sem=ssem, recv_sem=rsem,
            device_id={"row": row, "col": col}, device_id_type=pl.DeviceIdType.MESH,
        )
        if cond is None:
            copy.start()
        else:
            pl.when(cond)(copy.start)

    def later(size, ssem, cond=None):
        copy = pltpu.make_async_remote_copy(
            src_ref=size, dst_ref=size, send_sem=ssem, recv_sem=ssem,
            device_id={"row": r, "col": c}, device_id_type=pl.DeviceIdType.MESH,
        )
        pending.append((cond, copy))

    def drain():
        for cond, copy in pending:
            if cond is None:
                copy.wait_send()
            else:
                pl.when(cond)(copy.wait_send)
        pending.clear()

    def arrived(dst, rsem, cond=None):
        copy = pltpu.make_async_remote_copy(
            src_ref=dst, dst_ref=dst, send_sem=rsem, recv_sem=rsem,
            device_id={"row": r, "col": c}, device_id_type=pl.DeviceIdType.MESH,
        )
        if cond is None:
            copy.wait_recv()
        else:
            pl.when(cond)(copy.wait_recv)

    def x_row(step):
        return ring(x, step, NX) * NY + y

    def y_row(step):
        return x * NY + ring(y, step, NY)

    loads = [
        pltpu.make_async_copy(src, dst, in_s.at[i])
        for i, (src, dst) in enumerate(((p_hbm, p_ref), (l_hbm, l_ref), (s_hbm, s_ref), (d_hbm, d_ref)))
    ]
    for load in loads:
        load.start()

    stores = []

    def put(src, dst, k):
        store = pltpu.make_async_copy(src.at[k], dst.at[k], out_s.at[len(stores)])
        store.start()
        stores.append(store)

    barrier = pltpu.get_barrier_semaphore()

    def greet(row, col):
        pl.semaphore_signal(barrier, inc=1, device_id={"row": row, "col": col}, device_id_type=pl.DeviceIdType.MESH)

    for i in range(1, NX):
        greet(x_row(i), c)
    for i in range(1, NY):
        greet(y_row(i), c)
    for i in range(1, nc):
        greet(r, ring(c, i, nc))

    for i in range(NX):
        for j in range(cx):
            here = (i == x) & (xt == x) & (j == slot)
            pl.when(jnp.logical_not(here))(functools.partial(greet, i * NY + y, x * cx + j))

    lane = lax.broadcasted_iota(jnp.int32, (1, rows), 1)
    mask = jnp.zeros((1, rows), f32)
    for j in range(rows // TILE):
        tile = r * (rows // TILE) + j
        hit = jnp.float32(0)
        for i in range(tiles.shape[0]):
            hit = hit + jnp.where(tiles[i] == tile, 1.0, 0.0)
        inside = jnp.where((lane >= j * TILE) & (lane < (j + 1) * TILE), 1.0, 0.0)
        mask = mask + inside * hit

    sources = [2 * c, 2 * c + 1]
    dist = [lax.rem(y - lax.rem(src, NY) + NY, NY) for src in sources]
    reach = NY // 2 - 1 + core if NY == 8 else NY // 2
    hops = [jnp.where(d <= reach, d, NY - d) for d in dist]
    near = jnp.where(hops[1] < hops[0], 1, 0)
    order = []
    for src in (near, 1 - near):
        at = 2 * c + src
        xs_at = lax.div(at, NY)
        order.append((src, r == at, lax.rem(y - lax.rem(at, NY) + NY, NY), xs_at))

    loads[0].wait()
    for s in range(2):

        @pl.when(r == sources[s])
        def _():
            for k in range(SUPER):
                turned = p_ref[k].T * mask.astype(bf16)
                pt[k, s] = turned.reshape(NX, 2, lanes // 2, kb)

    pl.semaphore_wait(barrier, NX - 1 + NY - 1 + nc - 1 + nc - jnp.where(xt == x, 1, 0))

    def inject(k):
        for s, is_source, _, _ in order[:1]:
            for h in range(2):
                for i in (2, 1, 3) if NX == 4 else range(1, NX):
                    q = ring(x, i, NX)
                    here = pt.at[k, s, q, h]
                    send(here, here, psc_s.at[k], psa_r.at[k, s, h], x_row(i), c, is_source)
            later(pt.at[k, 0, : NX - 1], psc_s.at[k], is_source)

    def relay_links():
        arrived(cf.at[:, : nz - 1, core], c_r.at[0])
        send(cf.at[:, :, core], cf.at[:, :, core], cd_s.at[0], cd_r.at[0], r, z * 2 + other)
        later(cf.at[:, :, core], cd_s.at[0])

    def links_here():
        arrived(cf.at[:, :, other], cd_r.at[0])
        for k in range(SUPER - 1):
            ct[k] = cf[k].reshape(wide, wide).T.reshape(NX, lanes, wide)

    def pass_on(k):
        for j, (s, is_source, away, xq) in enumerate(order):
            for h in range(2):
                here = pt.at[k, s, x, h]
                arrived(here, psa_r.at[k, s, h], jnp.logical_not(is_source))
                for n, (senders, more_0, more_1, step) in enumerate(along(NY)):
                    sends = any_of(away, senders) | (away == jnp.where(core == 0, more_0, more_1))
                    send(here, here, psa_s.at[k, j], psa_r.at[k, s, h], y_row(step), c, sends)
                    once = sends if n == 0 else once | sends
                for i in (1, NX - 1) if NX > 2 else (1,):
                    to_source = (away == 0) & (ring(x, i, NX) == xq)
                    send(
                        here, here, psx_s.at[k, j], psx_r.at[k, s, h, i // 2], x_row(i), c, jnp.logical_not(to_source)
                    )
            later(pt.at[k, 0, : len(along(NY))], psa_s.at[k, j], away == 0)
            later(pt.at[k, 0, 0], psa_s.at[k, j], once & (away != 0))
            beside = (away == 0) & ((ring(x, 1, NX) == xq) | (ring(x, NX - 1, NX) == xq))
            later(pt.at[k, 0, : NX - 1], psx_s.at[k, j], jnp.logical_not(beside))
            if NX == 4:
                later(pt.at[k, 0, :3, 0], psx_s.at[k, j], beside)

    def forward(k):
        for j, (s, is_source, away, xq) in enumerate(order):
            needed = jnp.logical_not(is_source)
            for h in range(2):
                for i in (1, NX - 1) if NX > 2 else (1,):
                    there = pt.at[k, s, ring(x, NX - i, NX), h]
                    arrived(there, psx_r.at[k, s, h, i // 2], needed)
                    if NX == 4 and i == (1 if h == 0 else 3):
                        to_source = (away == 0) & (ring(x, i, NX) == xq)
                        send(
                            there, there, psx_s.at[k, j], psf_r.at[k, s], x_row(i), c,
                            jnp.logical_not(to_source),
                        )

    def panel_here(k):
        if NX == 4:
            for s, is_source, _, _ in order:
                arrived(pt.at[k, s, ring(x, 2, NX)], psf_r.at[k, s], jnp.logical_not(is_source))

    def two_terms():
        loads[2].wait()
        size = min(rows, 128)

        @pl.loop(0, rows // size)
        def _(j):
            here = pl.ds(pl.multiple_of(j * size, size), size)
            for s in range(2):
                high, low = halves(s_ref[here, s * kb : (s + 1) * kb])
                sh[s, here] = high
                sl[s, here] = low

    def share_links():
        loads[1].wait()
        for i in range(1, nz):
            send(l_ref, cf.at[:, z, core], c_s.at[0], c_r.at[0], r, ring(z, i, nz) * 2 + core)
        later(cf.at[:, : nz - 1, core], c_s.at[0])
        cf[:, z, core] = l_ref[...]

    zx = nz // NX

    def partial(k):
        two = 2 * lanes

        @pl.loop(0, NX // 2)
        def _(q):
            first = pt[k, 0, pl.ds(2 * q, 2)].reshape(two, kb)
            second = pt[k, 1, pl.ds(2 * q, 2)].reshape(two, kb)
            acc = dot_t(first, sh[0]) + dot_t(first, sl[0])
            acc = acc + dot_t(second, sh[1]) + dot_t(second, sl[1])
            if k > 0:
                factor = ct[k - 1, pl.ds(2 * q, 2)].reshape(two, wide)
                acc = acc + dot(factor, xh[k - 1]) + dot(factor, xl[k - 1])
            acc = -acc
            if k + 1 < SUPER:
                here = pl.ds(pl.multiple_of(q * two, two), two)
                high, low = halves(acc)
                xh[k, here] = high
                xl[k, here] = low
            xp[k, pl.ds(q * 2 * zx, 2 * zx)] = acc.reshape(2 * zx, 2, wc, rows)

        send(xp.at[k, :, other], xsib.at[k], d2_s.at[k], d2_r.at[k], r, z * 2 + other)
        later(xsib.at[k], d2_s.at[k])

    def along_z(k):
        arrived(xsib.at[k], d2_r.at[k])
        mine = xp[k, :, core] + xsib[k]
        own[k] = xp[k, z, core] + xsib[k, z]
        top = jnp.max(jnp.abs(mine), axis=1, keepdims=True)
        sc[k] = top * (1 / 32767)
        steps = jnp.where(top > 0, 32767 / jnp.where(top > 0, top, 1.0), 0.0)
        xs[k] = jnp.round(mine * steps).astype(jnp.int32).astype(jnp.int16)
        for i in range(1, nz):
            to = ring(z, i, nz)
            send(sc.at[k, to], sr.at[k, z], s_s.at[k], s_r.at[k], r, to * 2 + core)
            send(xs.at[k, to], xr.at[k, z], z_s.at[k], z_r.at[k], r, to * 2 + core)
        later(sc.at[k, : nz - 1], s_s.at[k])
        later(xs.at[k, : nz - 1], z_s.at[k])

    def summed(k):
        return wc if k + 1 == SUPER else 2 * wc

    def inverse_panel(k):
        total = own[k]
        arrived(sr.at[k, : nz - 1], s_r.at[k])
        arrived(xr.at[k, : nz - 1], z_r.at[k])
        for i in range(1, nz):
            src = ring(z, nz - i, nz)
            total = total + xr[k, src].astype(jnp.int32).astype(f32) * sr[k, src]
        total = total * mask
        x_out[k] = total
        put(x_out, x_hbm, k)
        high, low = halves(total)
        both = jnp.concatenate([high, low], axis=0)
        for j in range(k, min(k + 2, SUPER)):
            terms = dot(both, p_ref[j])
            at = (j - k) * wc
            ap[k, at : at + wc] = terms[:wc] + terms[wc:]
        n = summed(k)
        for i in range(1, NX):
            to = ring(x, i, NX)
            cut = pl.ds(pl.multiple_of(to * lanes, lanes), lanes)
            send(ap.at[k, :n, cut], ar.at[k, x, :n], ar_s.at[k], ar_r.at[k], x_row(i), c)
        later(ar.at[k, : NX - 1, :n], ar_s.at[k])

    def along_y(k):
        n = summed(k)
        total = ap[k, :n, my_lanes]
        arrived(ar.at[k, : NX - 1, :n], ar_r.at[k])
        for i in range(1, NX):
            src = ring(x, NX - i, NX)
            total = total + ar[k, src, :n]
        ax[k, :n] = total
        for i in range(1, NY):
            send(ax.at[k, :n], ay.at[k, y, :n], ay_s.at[k], ay_r.at[k], y_row(i), c)
        later(ay.at[k, : NY - 1, :n], ay_s.at[k])

    def products(k):
        n = summed(k)
        total = ax[k, :n]
        arrived(ay.at[k, : NY - 1, :n], ay_r.at[k])
        for i in range(1, NY):
            src = ring(y, NY - i, NY)
            total = total + ay[k, src, :n]
        bb[k, :n] = total
        ex[k, :, my_lanes] = total[:wc]
        for i in range(1, NX):
            send(bb.at[k, :wc], ex.at[k, :, my_lanes], ex_s.at[k], ex_r.at[k], x_row(i), c)
        later(ex.at[k, :, : (NX - 1) * lanes], ex_s.at[k])
        if k == 0:
            for i in range(nz):
                away = (xt != x) | (z != i)
                to = tf.at[x * (cx // 2) + lax.div(slot, 2), core]
                send(bb.at[k, wc:], to, tf_s.at[0], tf_r.at[0], xt * NY + y, i * 2 + core, away)
            later(tf.at[:, core], tf_s.at[0], xt != x)
            later(tf.at[: nz - 1, core], tf_s.at[0], xt == x)

            @pl.when(xt == x)
            def _():
                tf[x * (cx // 2) + lax.div(slot, 2), core] = bb[k, wc:]

        elif k + 1 < SUPER:
            for i in range(cx):
                away = (xt != x) | (slot != i)
                send(bb.at[k, wc:], tb.at[slot], t_s.at[0], t_r.at[0], xt * NY + y, x * cx + i, away)

                @pl.when(jnp.logical_not(away))
                def _():
                    tb[i] = bb[k, wc:]

            later(tb, t_s.at[0], xt != x)
            later(tb.at[: cx - 1], t_s.at[0], xt == x)

    def everyone(k):
        gx[k] = d_ref[k, :, my_lanes] - bb[k, :wc]
        for i in range(1, nz):
            send(gx.at[k], ga.at[k, z, core], ga_s.at[k], ga_r.at[k], r, ring(z, i, nz) * 2 + core)
        later(ga.at[k, : nz - 1, core], ga_s.at[k])
        ga[k, z, core] = gx[k]

    def relay(k):
        arrived(ga.at[k, : nz - 1, core], ga_r.at[k])
        send(ga.at[k, :, core], ga.at[k, :, core], gd_s.at[k], gd_r.at[k], r, z * 2 + other)
        later(ga.at[k, :, core], gd_s.at[k])
        if k == 0:
            arrived(tf.at[:, core], tf_r.at[0], xt != x)
            arrived(tf.at[: nz - 1, core], tf_r.at[0], xt == x)
            send(tf.at[:, core], tf.at[:, core], td_s.at[0], td_r.at[0], r, z * 2 + other)
            later(tf.at[:, core], td_s.at[0])

    def rows_of(k):
        return ct[k, xt, pl.ds(pl.multiple_of(slot * wc, wc), wc)]

    def cross(k):
        n = wc
        arrived(ga.at[k, :, other], gd_r.at[k])
        high, low = halves(ga[k].reshape(nc * wc, lanes))
        if k == 0:
            n = 2 * wc
            arrived(tf.at[:, other], td_r.at[0])
            for i in range(NX):
                turned = tf[i * (cx // 2) : (i + 1) * (cx // 2)].reshape(lanes, lanes).T
                total = -(turned + dot(ct[k, i], high) + dot(ct[k, i], low))
                ya[i] = total.reshape(cx, wc, lanes)
            yx[k, :wc] = ya[xt, slot]
            high, low = halves(ya[...].reshape(wide, lanes))
            yx[k, wc:] = dot(rows_of(1), high) + dot(rows_of(1), low)
        else:
            arrived(tb, t_r.at[0], xt != x)
            arrived(tb.at[: cx - 1], t_r.at[0], xt == x)
            tt[...] = tb[...].reshape(cx * wc, lanes).T.reshape(cx, wc, lanes)
            yx[k, :wc] = vc[:, my_lanes] - (tt[slot] + dot(rows_of(k), high) + dot(rows_of(k), low))
        yf[k, :n, my_lanes] = yx[k, :n]
        for i in range(1, NX):
            send(yx.at[k, :n], yf.at[k, :n, my_lanes], yx_s.at[k], yx_r.at[k], x_row(i), c)
        later(yf.at[k, :n, : (NX - 1) * lanes], yx_s.at[k])

    def gathered(ref, sems, k, n):
        arrived(ref.at[k, :n, : (NX - 1) * lanes], sems.at[k])
        return ref[k, :n]

    inject(0)
    share_links()
    pass_on(0)
    inject(1)
    two_terms()
    forward(0)
    pass_on(1)
    inject(2)
    panel_here(0)
    partial(0)
    relay_links()
    forward(1)
    along_z(0)
    links_here()
    pass_on(2)
    panel_here(1)
    partial(1)
    along_z(1)
    inverse_panel(0)
    forward(2)
    along_y(0)
    panel_here(2)
    partial(2)
    inverse_panel(1)
    along_z(2)
    loads[3].wait()
    along_y(1)
    products(0)
    everyone(0)
    inverse_panel(2)
    products(1)
    everyone(1)
    relay(0)
    cross(0)
    along_y(2)
    drain()
    g_out[0] = d_ref[0] - gathered(ex, ex_r, 0, wc)
    put(g_out, g_hbm, 0)
    y_out[0] = gathered(yf, yx_r, 0, 2 * wc)[:wc]
    put(y_out, y_hbm, 0)
    joined = left_dot(yf[0], cf[0].reshape(wide, wide))
    vc[...] = joined[wc:]
    g_out[1] = d_ref[1] - gathered(ex, ex_r, 1, wc) - joined[:wc]
    put(g_out, g_hbm, 1)
    relay(1)
    cross(1)
    products(2)
    drain()
    y_out[1] = gathered(yf, yx_r, 1, wc)
    put(y_out, y_hbm, 1)
    g_out[2] = d_ref[2] - gathered(ex, ex_r, 2, wc) - left_dot(y_out[1], cf[1].reshape(wide, wide))
    put(g_out, g_hbm, 2)
    drain()
    for store in stores:
        store.wait()


def finish(x_ref, y_ref, g_ref, x_out, y_out, g_out):
    x_out[...] = x_ref[...]
    y_out[...] = y_ref[...]
    g_out[...] = g_ref[...]


def local(nz, nc, inverse_block, tile_list, panels, links, diag_inverse):
    rows, depth = inverse_block.shape
    wide = panels.shape[2]
    wc = wide // nc
    lanes = wide // NX
    cx = nc // NX
    pair = SUPER - 1
    vmem = pl.BlockSpec(memory_space=pltpu.VMEM)
    dma = pltpu.SemaphoreType.DMA
    x, y, g = pl.pallas_call(
        functools.partial(kernel, nz, nc),
        out_shape=(
            jax.ShapeDtypeStruct((SUPER, wc, rows), f32),
            jax.ShapeDtypeStruct((pair, wc, wide), f32),
            jax.ShapeDtypeStruct((SUPER, wc, wide), f32),
        ),
        in_specs=[pl.BlockSpec(memory_space=pltpu.SMEM)] + [pl.BlockSpec(memory_space=pl.ANY)] * 4,
        out_specs=(pl.BlockSpec(memory_space=pl.ANY),) * 3,
        scratch_shapes=[
            pltpu.VMEM((rows, depth), f32),
            pltpu.VMEM(panels.shape, bf16),
            pltpu.VMEM(links.shape, bf16),
            pltpu.VMEM((SUPER, wc, wide), f32),
            pltpu.VMEM((SUPER, wc, rows), f32),
            pltpu.VMEM((pair, wc, wide), f32),
            pltpu.VMEM((SUPER, wc, wide), f32),
            dma((4,)),
            dma((3 * SUPER - 1,)),
            pltpu.VMEM((2, rows, depth // 2), bf16),
            pltpu.VMEM((2, rows, depth // 2), bf16),
            pltpu.VMEM((SUPER, 2, NX, 2, lanes // 2, depth // 2), bf16),
            pltpu.VMEM((SUPER, nz, 2, wc, rows), f32),
            pltpu.VMEM((pair, wide, rows), bf16),
            pltpu.VMEM((pair, wide, rows), bf16),
            pltpu.VMEM((SUPER, nz, wc, rows), f32),
            pltpu.VMEM((SUPER, nz, wc, rows), jnp.int16),
            pltpu.VMEM((SUPER, nz, wc, rows), jnp.int16),
            pltpu.VMEM((SUPER, wc, rows), f32),
            pltpu.VMEM((SUPER, nz, 1, rows), f32),
            pltpu.VMEM((SUPER, nz, 1, rows), f32),
            pltpu.VMEM((pair, nz, 2, wc, wide), bf16),
            pltpu.VMEM((pair, NX, lanes, wide), bf16),
            pltpu.VMEM((SUPER, 2 * wc, wide), f32),
            pltpu.VMEM((SUPER, NX, 2 * wc, lanes), f32),
            pltpu.VMEM((SUPER, 2 * wc, lanes), f32),
            pltpu.VMEM((SUPER, NY, 2 * wc, lanes), f32),
            pltpu.VMEM((SUPER, 2 * wc, lanes), f32),
            pltpu.VMEM((SUPER, wc, wide), f32),
            pltpu.VMEM((cx, wc, lanes), f32),
            pltpu.VMEM((nz, 2, wc, lanes), f32),
            pltpu.VMEM((cx, wc, lanes), f32),
            pltpu.VMEM((pair, wc, lanes), f32),
            pltpu.VMEM((pair, nz, 2, wc, lanes), f32),
            pltpu.VMEM((NX, cx, wc, lanes), f32),
            pltpu.VMEM((pair, 2 * wc, lanes), f32),
            pltpu.VMEM((pair, 2 * wc, wide), f32),
            pltpu.VMEM((wc, wide), f32),
            dma((SUPER, 2)),
            dma((SUPER,)),
            dma((SUPER, 2)),
            dma((SUPER, 2, 2)),
            dma((SUPER, 2, 2, 2)),
            dma((SUPER, 2)),
            dma((1,)), dma((1,)),
            dma((1,)), dma((1,)),
            dma((SUPER,)), dma((SUPER,)),
            dma((SUPER,)), dma((SUPER,)),
            dma((SUPER,)), dma((SUPER,)),
            dma((SUPER,)), dma((SUPER,)),
            dma((SUPER,)), dma((SUPER,)),
            dma((SUPER,)), dma((SUPER,)),
            dma((1,)), dma((1,)),
            dma((1,)), dma((1,)),
            dma((1,)), dma((1,)),
            dma((pair,)), dma((pair,)),
            dma((pair,)), dma((pair,)),
            dma((pair,)), dma((pair,)),
        ],
        compiler_params=pltpu.CompilerParams(
            collective_id=0, has_side_effects=True, vmem_limit_bytes=60 * 1024 * 1024
        ),
    )(tile_list, inverse_block, panels, links, jnp.swapaxes(diag_inverse, 1, 2))
    x, y, g = pl.pallas_call(
        finish,
        out_shape=tuple(jax.ShapeDtypeStruct(value.shape, f32) for value in (x, y, g)),
        in_specs=[vmem] * 3,
        out_specs=(vmem,) * 3,
    )(x, y, g)
    return tuple(jnp.swapaxes(value, 1, 2) for value in (x, y, g))


def solution(mesh):
    nc = mesh.shape["col"]
    return jax.shard_map(
        functools.partial(local, nc // 2, nc),
        mesh=mesh,
        in_specs=(
            P("row", "col"),
            P(),
            P(None, "row", None),
            P(None, "col", None),
            P(None, None, "col"),
        ),
        out_specs=(P(None, "row", "col"), P(None, None, "col"), P(None, None, "col")),
        check_vma=False,
    )
```

```python
import functools

import jax
import jax.numpy as jnp
from jax import lax
from jax.experimental import pallas as pl
from jax.experimental.pallas import tpu as pltpu
from jax.sharding import PartitionSpec as P

NX = 4
NY = 8
TILE = 256
SUPER = 3
f32 = jnp.float32
bf16 = jnp.bfloat16


def halves(value):
    high = value.astype(bf16)
    low = (value - high.astype(f32)).astype(bf16)
    return high, low


def dot(left, right):
    return lax.dot_general(left, right, (((1,), (0,)), ((), ())), preferred_element_type=f32)


def dot_t(left, right):
    return lax.dot_general(left, right, (((1,), (1,)), ((), ())), preferred_element_type=f32)


def left_dot(left, right):
    high, low = halves(left)
    both = dot(jnp.concatenate([high, low], axis=0), right)
    return both[: left.shape[0]] + both[left.shape[0] :]


def along(size):
    if size == 8:
        return (((0,), 0, 0, 3), ((0,), 0, 0, 6), ((0, 1, 3), 0, 0, 1), ((0, 6), 0, 0, 7))
    return (((0, 1), 0, 0, 1), ((0,), 0, 0, 3))


def far_first(size):
    return sorted(range(1, size), key=lambda i: -min(i, size - i))


def any_of(value, choices):
    hit = value == choices[0]
    for choice in choices[1:]:
        hit = hit | (value == choice)
    return hit


def kernel(
    nz, nc, tiles, s_hbm, p_hbm, l_hbm, d_hbm, x_hbm, y_hbm, g_hbm,
    s_ref, p_ref, l_ref, d_ref, x_out, y_out, g_out, in_s, out_s,
    sh, sl, pt, xp, xh, xl, xsib, xs, xr, own, sc, sr, cf, ct, ap, ar, ax, ay, bb, ex, tb, tf, tt, gx, ga, ya, yx, yf, vc,
    psa_s, psc_s, psx_s, psa_r, psx_r, psf_r, c_s, c_r, cd_s, cd_r, d2_s, d2_r, z_s, z_r, s_s, s_r,
    ar_s, ar_r, ay_s, ay_r, ex_s, ex_r, t_s, t_r, tf_s, tf_r, td_s, td_r, ga_s, ga_r, gd_s, gd_r, yx_s, yx_r,
):
    rows, depth = s_ref.shape
    wide = p_ref.shape[2]
    wc = wide // nc
    lanes = wide // NX
    cx = nc // NX
    kb = depth // 2
    r = lax.axis_index("row")
    c = lax.axis_index("col")
    x, y = lax.div(r, NY), lax.rem(r, NY)
    z, core = lax.div(c, 2), lax.rem(c, 2)
    other = 1 - core
    xt, slot = lax.div(c, cx), lax.rem(c, cx)
    my_lanes = pl.ds(pl.multiple_of(x * lanes, lanes), lanes)

    def ring(at, step, size):
        return lax.rem(at + step, size)

    pending = []

    def send(src, dst, ssem, rsem, row, col, cond=None):
        copy = pltpu.make_async_remote_copy(
            src_ref=src, dst_ref=dst, send_sem=ssem, recv_sem=rsem,
            device_id={"row": row, "col": col}, device_id_type=pl.DeviceIdType.MESH,
        )
        if cond is None:
            copy.start()
        else:
            pl.when(cond)(copy.start)

    def later(size, ssem, cond=None):
        copy = pltpu.make_async_remote_copy(
            src_ref=size, dst_ref=size, send_sem=ssem, recv_sem=ssem,
            device_id={"row": r, "col": c}, device_id_type=pl.DeviceIdType.MESH,
        )
        pending.append((cond, copy))

    def drain():
        for cond, copy in pending:
            if cond is None:
                copy.wait_send()
            else:
                pl.when(cond)(copy.wait_send)
        pending.clear()

    def arrived(dst, rsem, cond=None):
        copy = pltpu.make_async_remote_copy(
            src_ref=dst, dst_ref=dst, send_sem=rsem, recv_sem=rsem,
            device_id={"row": r, "col": c}, device_id_type=pl.DeviceIdType.MESH,
        )
        if cond is None:
            copy.wait_recv()
        else:
            pl.when(cond)(copy.wait_recv)

    def x_row(step):
        return ring(x, step, NX) * NY + y

    def y_row(step):
        return x * NY + ring(y, step, NY)

    loads = [
        pltpu.make_async_copy(src, dst, in_s.at[i])
        for i, (src, dst) in enumerate(((p_hbm, p_ref), (l_hbm, l_ref), (s_hbm, s_ref), (d_hbm, d_ref)))
    ]
    for load in loads:
        load.start()

    stores = []

    def put(src, dst, k):
        store = pltpu.make_async_copy(src.at[k], dst.at[k], out_s.at[len(stores)])
        store.start()
        stores.append(store)

    barrier = pltpu.get_barrier_semaphore()

    def greet(row, col):
        pl.semaphore_signal(barrier, inc=1, device_id={"row": row, "col": col}, device_id_type=pl.DeviceIdType.MESH)

    for i in range(1, NX):
        greet(x_row(i), c)
    for i in range(1, NY):
        greet(y_row(i), c)
    for i in range(1, nc):
        greet(r, ring(c, i, nc))

    for i in range(NX):
        for j in range(cx):
            here = (i == x) & (xt == x) & (j == slot)
            pl.when(jnp.logical_not(here))(functools.partial(greet, i * NY + y, x * cx + j))

    lane = lax.broadcasted_iota(jnp.int32, (1, rows), 1)
    mask = jnp.zeros((1, rows), f32)
    for j in range(rows // TILE):
        tile = r * (rows // TILE) + j
        hit = jnp.float32(0)
        for i in range(tiles.shape[0]):
            hit = hit + jnp.where(tiles[i] == tile, 1.0, 0.0)
        inside = jnp.where((lane >= j * TILE) & (lane < (j + 1) * TILE), 1.0, 0.0)
        mask = mask + inside * hit

    sources = [2 * c, 2 * c + 1]
    dist = [lax.rem(y - lax.rem(src, NY) + NY, NY) for src in sources]
    reach = NY // 2
    hops = [jnp.where(d <= reach, d, NY - d) for d in dist]
    near = jnp.where(hops[1] < hops[0], 1, 0)
    order = []
    for src in (near, 1 - near):
        at = 2 * c + src
        xs_at = lax.div(at, NY)
        order.append((src, r == at, lax.rem(y - lax.rem(at, NY) + NY, NY), xs_at))

    loads[0].wait()
    for s in range(2):

        @pl.when(r == sources[s])
        def _():
            for k in range(SUPER):
                turned = p_ref[k].T * mask.astype(bf16)
                pt[k, s] = turned.reshape(NX, 2, lanes // 2, kb)

    pl.semaphore_wait(barrier, NX - 1 + NY - 1 + nc - 1 + nc - jnp.where(xt == x, 1, 0))

    def inject(k):
        for s, is_source, _, _ in order[:1]:
            for h in range(2):
                for i in (2, 1, 3) if NX == 4 else range(1, NX):
                    q = ring(x, i, NX)
                    here = pt.at[k, s, q, h]
                    send(here, here, psc_s.at[k], psa_r.at[k, s, h], x_row(i), c, is_source)
            later(pt.at[k, 0, : NX - 1], psc_s.at[k], is_source)

    def relay_links():
        arrived(cf.at[:, : nz - 1, core], c_r.at[0])
        send(cf.at[:, :, core], cf.at[:, :, core], cd_s.at[0], cd_r.at[0], r, z * 2 + other)
        later(cf.at[:, :, core], cd_s.at[0])

    def links_here():
        arrived(cf.at[:, :, other], cd_r.at[0])
        for k in range(SUPER - 1):
            ct[k] = cf[k].reshape(wide, wide).T.reshape(NX, lanes, wide)

    def pass_on(k):
        for j, (s, is_source, away, xq) in enumerate(order):
            for h in range(2):
                here = pt.at[k, s, x, h]
                arrived(here, psa_r.at[k, s, h], jnp.logical_not(is_source))
                for n, (senders, more_0, more_1, step) in enumerate(along(NY)):
                    sends = any_of(away, senders) | (away == jnp.where(core == 0, more_0, more_1))
                    send(here, here, psa_s.at[k, j], psa_r.at[k, s, h], y_row(step), c, sends)
                    once = sends if n == 0 else once | sends
                for i in (1, NX - 1) if NX > 2 else (1,):
                    to_source = (away == 0) & (ring(x, i, NX) == xq)
                    send(
                        here, here, psx_s.at[k, j], psx_r.at[k, s, h, i // 2], x_row(i), c, jnp.logical_not(to_source)
                    )
            later(pt.at[k, 0, : len(along(NY))], psa_s.at[k, j], away == 0)
            later(pt.at[k, 0, 0], psa_s.at[k, j], once & (away != 0))
            beside = (away == 0) & ((ring(x, 1, NX) == xq) | (ring(x, NX - 1, NX) == xq))
            later(pt.at[k, 0, : NX - 1], psx_s.at[k, j], jnp.logical_not(beside))
            if NX == 4:
                later(pt.at[k, 0, :3, 0], psx_s.at[k, j], beside)

    def forward(k):
        for j, (s, is_source, away, xq) in enumerate(order):
            needed = jnp.logical_not(is_source)
            for h in range(2):
                for i in (1, NX - 1) if NX > 2 else (1,):
                    there = pt.at[k, s, ring(x, NX - i, NX), h]
                    arrived(there, psx_r.at[k, s, h, i // 2], needed)
                    if NX == 4 and i == (1 if h == 0 else 3):
                        to_source = (away == 0) & (ring(x, i, NX) == xq)
                        send(
                            there, there, psx_s.at[k, j], psf_r.at[k, s], x_row(i), c,
                            jnp.logical_not(to_source),
                        )

    def panel_here(k):
        if NX == 4:
            for s, is_source, _, _ in order:
                arrived(pt.at[k, s, ring(x, 2, NX)], psf_r.at[k, s], jnp.logical_not(is_source))

    def two_terms():
        loads[2].wait()
        size = min(rows, 128)

        @pl.loop(0, rows // size)
        def _(j):
            here = pl.ds(pl.multiple_of(j * size, size), size)
            for s in range(2):
                high, low = halves(s_ref[here, s * kb : (s + 1) * kb])
                sh[s, here] = high
                sl[s, here] = low

    def share_links():
        loads[1].wait()
        for i in range(1, nz):
            send(l_ref, cf.at[:, z, core], c_s.at[0], c_r.at[0], r, ring(z, i, nz) * 2 + core)
        later(cf.at[:, : nz - 1, core], c_s.at[0])
        cf[:, z, core] = l_ref[...]

    zx = nz // NX

    def partial(k):
        two = 2 * lanes

        @pl.loop(0, NX // 2)
        def _(q):
            first = pt[k, 0, pl.ds(2 * q, 2)].reshape(two, kb)
            second = pt[k, 1, pl.ds(2 * q, 2)].reshape(two, kb)
            acc = dot_t(first, sh[0]) + dot_t(first, sl[0])
            acc = acc + dot_t(second, sh[1]) + dot_t(second, sl[1])
            if k > 0:
                factor = ct[k - 1, pl.ds(2 * q, 2)].reshape(two, wide)
                acc = acc + dot(factor, xh[k - 1]) + dot(factor, xl[k - 1])
            acc = -acc
            if k + 1 < SUPER:
                here = pl.ds(pl.multiple_of(q * two, two), two)
                high, low = halves(acc)
                xh[k, here] = high
                xl[k, here] = low
            xp[k, pl.ds(q * 2 * zx, 2 * zx)] = acc.reshape(2 * zx, 2, wc, rows)

        send(xp.at[k, :, other], xsib.at[k], d2_s.at[k], d2_r.at[k], r, z * 2 + other)
        later(xsib.at[k], d2_s.at[k])

    def along_z(k):
        arrived(xsib.at[k], d2_r.at[k])
        mine = xp[k, :, core] + xsib[k]
        own[k] = xp[k, z, core] + xsib[k, z]
        top = jnp.max(jnp.abs(mine), axis=1, keepdims=True)
        sc[k] = top * (1 / 32767)
        steps = jnp.where(top > 0, 32767 / jnp.where(top > 0, top, 1.0), 0.0)
        xs[k] = jnp.round(mine * steps).astype(jnp.int32).astype(jnp.int16)
        for i in far_first(nz):
            to = ring(z, i, nz)
            send(sc.at[k, to], sr.at[k, z], s_s.at[k], s_r.at[k], r, to * 2 + core)
            send(xs.at[k, to], xr.at[k, z], z_s.at[k], z_r.at[k], r, to * 2 + core)
        later(sc.at[k, : nz - 1], s_s.at[k])
        later(xs.at[k, : nz - 1], z_s.at[k])

    def summed(k):
        return wc if k + 1 == SUPER else 2 * wc

    def inverse_panel(k):
        total = own[k]
        arrived(sr.at[k, : nz - 1], s_r.at[k])
        arrived(xr.at[k, : nz - 1], z_r.at[k])
        for i in range(1, nz):
            src = ring(z, nz - i, nz)
            total = total + xr[k, src].astype(jnp.int32).astype(f32) * sr[k, src]
        total = total * mask
        x_out[k] = total
        put(x_out, x_hbm, k)
        high, low = halves(total)
        both = jnp.concatenate([high, low], axis=0)
        for j in range(k, min(k + 2, SUPER)):
            terms = dot(both, p_ref[j])
            at = (j - k) * wc
            ap[k, at : at + wc] = terms[:wc] + terms[wc:]
        n = summed(k)
        for i in range(1, NX):
            to = ring(x, i, NX)
            cut = pl.ds(pl.multiple_of(to * lanes, lanes), lanes)
            send(ap.at[k, :n, cut], ar.at[k, x, :n], ar_s.at[k], ar_r.at[k], x_row(i), c)
        later(ar.at[k, : NX - 1, :n], ar_s.at[k])

    def along_y(k):
        n = summed(k)
        total = ap[k, :n, my_lanes]
        arrived(ar.at[k, : NX - 1, :n], ar_r.at[k])
        for i in range(1, NX):
            src = ring(x, NX - i, NX)
            total = total + ar[k, src, :n]
        ax[k, :n] = total
        for i in far_first(NY):
            send(ax.at[k, :n], ay.at[k, y, :n], ay_s.at[k], ay_r.at[k], y_row(i), c)
        later(ay.at[k, : NY - 1, :n], ay_s.at[k])

    def products(k):
        n = summed(k)
        total = ax[k, :n]
        arrived(ay.at[k, : NY - 1, :n], ay_r.at[k])
        for i in range(1, NY):
            src = ring(y, NY - i, NY)
            total = total + ay[k, src, :n]
        bb[k, :n] = total
        ex[k, :, my_lanes] = total[:wc]
        for i in range(1, NX):
            send(bb.at[k, :wc], ex.at[k, :, my_lanes], ex_s.at[k], ex_r.at[k], x_row(i), c)
        later(ex.at[k, :, : (NX - 1) * lanes], ex_s.at[k])
        if k == 0:
            for i in range(nz):
                away = (xt != x) | (z != i)
                to = tf.at[x * (cx // 2) + lax.div(slot, 2), core]
                send(bb.at[k, wc:], to, tf_s.at[0], tf_r.at[0], xt * NY + y, i * 2 + core, away)
            later(tf.at[:, core], tf_s.at[0], xt != x)
            later(tf.at[: nz - 1, core], tf_s.at[0], xt == x)

            @pl.when(xt == x)
            def _():
                tf[x * (cx // 2) + lax.div(slot, 2), core] = bb[k, wc:]

        elif k + 1 < SUPER:
            for i in range(cx):
                away = (xt != x) | (slot != i)
                send(bb.at[k, wc:], tb.at[slot], t_s.at[0], t_r.at[0], xt * NY + y, x * cx + i, away)

                @pl.when(jnp.logical_not(away))
                def _():
                    tb[i] = bb[k, wc:]

            later(tb, t_s.at[0], xt != x)
            later(tb.at[: cx - 1], t_s.at[0], xt == x)

    def everyone(k):
        gx[k] = d_ref[k, :, my_lanes] - bb[k, :wc]
        for i in far_first(nz):
            send(gx.at[k], ga.at[k, z, core], ga_s.at[k], ga_r.at[k], r, ring(z, i, nz) * 2 + core)
        later(ga.at[k, : nz - 1, core], ga_s.at[k])
        ga[k, z, core] = gx[k]

    def relay(k):
        arrived(ga.at[k, : nz - 1, core], ga_r.at[k])
        send(ga.at[k, :, core], ga.at[k, :, core], gd_s.at[k], gd_r.at[k], r, z * 2 + other)
        later(ga.at[k, :, core], gd_s.at[k])
        if k == 0:
            arrived(tf.at[:, core], tf_r.at[0], xt != x)
            arrived(tf.at[: nz - 1, core], tf_r.at[0], xt == x)
            send(tf.at[:, core], tf.at[:, core], td_s.at[0], td_r.at[0], r, z * 2 + other)
            later(tf.at[:, core], td_s.at[0])

    def rows_of(k):
        return ct[k, xt, pl.ds(pl.multiple_of(slot * wc, wc), wc)]

    def cross(k):
        n = wc
        arrived(ga.at[k, :, other], gd_r.at[k])
        high, low = halves(ga[k].reshape(nc * wc, lanes))
        if k == 0:
            n = 2 * wc
            arrived(tf.at[:, other], td_r.at[0])
            for i in range(NX):
                turned = tf[i * (cx // 2) : (i + 1) * (cx // 2)].reshape(lanes, lanes).T
                total = -(turned + dot(ct[k, i], high) + dot(ct[k, i], low))
                ya[i] = total.reshape(cx, wc, lanes)
            yx[k, :wc] = ya[xt, slot]
            high, low = halves(ya[...].reshape(wide, lanes))
            yx[k, wc:] = dot(rows_of(1), high) + dot(rows_of(1), low)
        else:
            arrived(tb, t_r.at[0], xt != x)
            arrived(tb.at[: cx - 1], t_r.at[0], xt == x)
            tt[...] = tb[...].reshape(cx * wc, lanes).T.reshape(cx, wc, lanes)
            yx[k, :wc] = vc[:, my_lanes] - (tt[slot] + dot(rows_of(k), high) + dot(rows_of(k), low))
        yf[k, :n, my_lanes] = yx[k, :n]
        for i in range(1, NX):
            send(yx.at[k, :n], yf.at[k, :n, my_lanes], yx_s.at[k], yx_r.at[k], x_row(i), c)
        later(yf.at[k, :n, : (NX - 1) * lanes], yx_s.at[k])

    def gathered(ref, sems, k, n):
        arrived(ref.at[k, :n, : (NX - 1) * lanes], sems.at[k])
        return ref[k, :n]

    inject(0)
    share_links()
    pass_on(0)
    inject(1)
    two_terms()
    forward(0)
    pass_on(1)
    inject(2)
    panel_here(0)
    partial(0)
    relay_links()
    forward(1)
    along_z(0)
    links_here()
    pass_on(2)
    panel_here(1)
    partial(1)
    inverse_panel(0)
    along_z(1)
    forward(2)
    along_y(0)
    panel_here(2)
    partial(2)
    inverse_panel(1)
    along_z(2)
    loads[3].wait()
    products(0)
    everyone(0)
    along_y(1)
    inverse_panel(2)
    products(1)
    everyone(1)
    relay(0)
    along_y(2)
    cross(0)
    drain()
    g_out[0] = d_ref[0] - gathered(ex, ex_r, 0, wc)
    put(g_out, g_hbm, 0)
    y_out[0] = gathered(yf, yx_r, 0, 2 * wc)[:wc]
    put(y_out, y_hbm, 0)
    joined = left_dot(yf[0], cf[0].reshape(wide, wide))
    vc[...] = joined[wc:]
    g_out[1] = d_ref[1] - gathered(ex, ex_r, 1, wc) - joined[:wc]
    put(g_out, g_hbm, 1)
    relay(1)
    cross(1)
    products(2)
    drain()
    y_out[1] = gathered(yf, yx_r, 1, wc)
    put(y_out, y_hbm, 1)
    g_out[2] = d_ref[2] - gathered(ex, ex_r, 2, wc) - left_dot(y_out[1], cf[1].reshape(wide, wide))
    put(g_out, g_hbm, 2)
    drain()
    for store in stores:
        store.wait()


def finish(x_ref, y_ref, g_ref, x_out, y_out, g_out):
    x_out[...] = x_ref[...]
    y_out[...] = y_ref[...]
    g_out[...] = g_ref[...]


def local(nz, nc, inverse_block, tile_list, panels, links, diag_inverse):
    rows, depth = inverse_block.shape
    wide = panels.shape[2]
    wc = wide // nc
    lanes = wide // NX
    cx = nc // NX
    pair = SUPER - 1
    vmem = pl.BlockSpec(memory_space=pltpu.VMEM)
    dma = pltpu.SemaphoreType.DMA
    x, y, g = pl.pallas_call(
        functools.partial(kernel, nz, nc),
        out_shape=(
            jax.ShapeDtypeStruct((SUPER, wc, rows), f32),
            jax.ShapeDtypeStruct((pair, wc, wide), f32),
            jax.ShapeDtypeStruct((SUPER, wc, wide), f32),
        ),
        in_specs=[pl.BlockSpec(memory_space=pltpu.SMEM)] + [pl.BlockSpec(memory_space=pl.ANY)] * 4,
        out_specs=(pl.BlockSpec(memory_space=pl.ANY),) * 3,
        scratch_shapes=[
            pltpu.VMEM((rows, depth), f32),
            pltpu.VMEM(panels.shape, bf16),
            pltpu.VMEM(links.shape, bf16),
            pltpu.VMEM((SUPER, wc, wide), f32),
            pltpu.VMEM((SUPER, wc, rows), f32),
            pltpu.VMEM((pair, wc, wide), f32),
            pltpu.VMEM((SUPER, wc, wide), f32),
            dma((4,)),
            dma((3 * SUPER - 1,)),
            pltpu.VMEM((2, rows, depth // 2), bf16),
            pltpu.VMEM((2, rows, depth // 2), bf16),
            pltpu.VMEM((SUPER, 2, NX, 2, lanes // 2, depth // 2), bf16),
            pltpu.VMEM((SUPER, nz, 2, wc, rows), f32),
            pltpu.VMEM((pair, wide, rows), bf16),
            pltpu.VMEM((pair, wide, rows), bf16),
            pltpu.VMEM((SUPER, nz, wc, rows), f32),
            pltpu.VMEM((SUPER, nz, wc, rows), jnp.int16),
            pltpu.VMEM((SUPER, nz, wc, rows), jnp.int16),
            pltpu.VMEM((SUPER, wc, rows), f32),
            pltpu.VMEM((SUPER, nz, 1, rows), f32),
            pltpu.VMEM((SUPER, nz, 1, rows), f32),
            pltpu.VMEM((pair, nz, 2, wc, wide), bf16),
            pltpu.VMEM((pair, NX, lanes, wide), bf16),
            pltpu.VMEM((SUPER, 2 * wc, wide), f32),
            pltpu.VMEM((SUPER, NX, 2 * wc, lanes), f32),
            pltpu.VMEM((SUPER, 2 * wc, lanes), f32),
            pltpu.VMEM((SUPER, NY, 2 * wc, lanes), f32),
            pltpu.VMEM((SUPER, 2 * wc, lanes), f32),
            pltpu.VMEM((SUPER, wc, wide), f32),
            pltpu.VMEM((cx, wc, lanes), f32),
            pltpu.VMEM((nz, 2, wc, lanes), f32),
            pltpu.VMEM((cx, wc, lanes), f32),
            pltpu.VMEM((pair, wc, lanes), f32),
            pltpu.VMEM((pair, nz, 2, wc, lanes), f32),
            pltpu.VMEM((NX, cx, wc, lanes), f32),
            pltpu.VMEM((pair, 2 * wc, lanes), f32),
            pltpu.VMEM((pair, 2 * wc, wide), f32),
            pltpu.VMEM((wc, wide), f32),
            dma((SUPER, 2)),
            dma((SUPER,)),
            dma((SUPER, 2)),
            dma((SUPER, 2, 2)),
            dma((SUPER, 2, 2, 2)),
            dma((SUPER, 2)),
            dma((1,)), dma((1,)),
            dma((1,)), dma((1,)),
            dma((SUPER,)), dma((SUPER,)),
            dma((SUPER,)), dma((SUPER,)),
            dma((SUPER,)), dma((SUPER,)),
            dma((SUPER,)), dma((SUPER,)),
            dma((SUPER,)), dma((SUPER,)),
            dma((SUPER,)), dma((SUPER,)),
            dma((1,)), dma((1,)),
            dma((1,)), dma((1,)),
            dma((1,)), dma((1,)),
            dma((pair,)), dma((pair,)),
            dma((pair,)), dma((pair,)),
            dma((pair,)), dma((pair,)),
        ],
        compiler_params=pltpu.CompilerParams(
            collective_id=0, has_side_effects=True, vmem_limit_bytes=60 * 1024 * 1024
        ),
    )(tile_list, inverse_block, panels, links, jnp.swapaxes(diag_inverse, 1, 2))
    x, y, g = pl.pallas_call(
        finish,
        out_shape=tuple(jax.ShapeDtypeStruct(value.shape, f32) for value in (x, y, g)),
        in_specs=[vmem] * 3,
        out_specs=(vmem,) * 3,
    )(x, y, g)
    return tuple(jnp.swapaxes(value, 1, 2) for value in (x, y, g))


def solution(mesh):
    nc = mesh.shape["col"]
    return jax.shard_map(
        functools.partial(local, nc // 2, nc),
        mesh=mesh,
        in_specs=(
            P("row", "col"),
            P(),
            P(None, "row", None),
            P(None, "col", None),
            P(None, None, "col"),
        ),
        out_specs=(P(None, "row", "col"), P(None, None, "col"), P(None, None, "col")),
        check_vma=False,
    )
```
